8 devices in a mesh: rep: 1 (over z), r: 2 (over y), s: 4 (over x, core).
Axes of the slice: x: 2, y: 2, z: 1, core: 2. Of those that a mesh axis runs over, the one named last changes fastest.
Arguments:
- x: bfloat16 [8, 4096, 512], P(('rep', 'r', 's'))
- dy: bfloat16 [8, 4096, 512], P(('rep', 'r', 's'))
- w_gate: bfloat16 [2, 512, 8192], P(None, 's')
- w_up: bfloat16 [2, 512, 8192], P(None, 's')
- w_down: bfloat16 [2, 8192, 512], P(None, 's')
- m_w_gate: float32 [2, 512, 8192], P(None, 's')
- m_w_up: float32 [2, 512, 8192], P(None, 's')
- m_w_down: float32 [2, 8192, 512], P(None, 's')
- v_w_gate: float32 [2, 512, 8192], P(None, 's')
- v_w_up: float32 [2, 512, 8192], P(None, 's')
- v_w_down: float32 [2, 8192, 512], P(None, 's')
Outputs:
- output 1: bfloat16 [2, 512, 8192], P('rep', 's')
- output 2: bfloat16 [2, 512, 8192], P('rep', 's')
- output 3: bfloat16 [2, 8192, 512], P('rep', 's')
- output 4: float32 [2, 512, 8192], P('rep', 's')
- output 5: float32 [2, 512, 8192], P('rep', 's')
- output 6: float32 [2, 8192, 512], P('rep', 's')
- output 7: float32 [2, 512, 8192], P('rep', 's')
- output 8: float32 [2, 512, 8192], P('rep', 's')
- output 9: float32 [2, 8192, 512], P('rep', 's')
All inputs are finite; a program needn't handle non-finite values.
Results may differ from the reference program's by a relative error of at most 0.0229.
Values are sent between devices in bfloat16 or wider.
A program may use at most 2 GiB of HBM per device.

```python
import jax
import jax.numpy as jnp
from jax import lax

SEQUENCES = 8
TOKENS = 4096
D = 512
FF = 8192
LAYERS = 2
NAMES = ("w_gate", "w_up", "w_down")
SHAPES = {"w_gate": (LAYERS, D, FF), "w_up": (LAYERS, D, FF), "w_down": (LAYERS, FF, D)}


def bump(key, n, height):
    away = (jnp.arange(n, dtype=jnp.int32) - jax.random.randint(key, (), 0, n, jnp.int32)) % n
    return jnp.where(away < n // 8, height, 1.0)


def together(key, own, strength):
    shared = jax.random.normal(key, own.shape[1:], jnp.float32)
    return (own + strength * shared) * lax.rsqrt(1 + strength * strength)


def setup_inputs(seed: int = 0, part: int = 0) -> dict:
    kx, kdy, ka, kb, kz, kf, kh, kl, *keys = jax.random.split(jax.random.key(seed), 8 + 3 * len(NAMES))
    kx, kdy, ka, kb = (jax.random.fold_in(k, part) for k in (kx, kdy, ka, kb))
    kw, km, kv = (keys[i::3] for i in range(3))
    shape = (SEQUENCES, TOKENS, D)
    much_x, much_dy = jax.random.uniform(kz, (2,), jnp.float32, 0.0, 1.0)
    loud = 2.0 ** jax.random.uniform(jax.random.fold_in(kz, 1), (), jnp.float32, -1.0, 2.0)
    layers = 2.0 ** jax.random.uniform(kl, (LAYERS, 1, 1), jnp.float32, -1.0, 1.0)
    x = together(ka, jax.random.normal(kx, shape, jnp.float32), much_x) * bump(kf, D, 4.0)
    dy = together(kb, jax.random.normal(kdy, shape, jnp.float32), much_dy)
    drawn = {"x": x.astype(jnp.bfloat16), "dy": (loud * dy * (SEQUENCES * TOKENS) ** -0.5).astype(jnp.bfloat16)}
    for key, name in zip(kw, NAMES, strict=True):
        w = jax.random.normal(key, SHAPES[name], jnp.float32) * SHAPES[name][1] ** -0.5
        drawn[name] = (w * {"w_gate": 1.0, "w_up": bump(kh, FF, 4.0), "w_down": layers}[name]).astype(jnp.bfloat16)
    for key, name in zip(km, NAMES, strict=True):
        drawn[f"m_{name}"] = 0.1 * jax.random.normal(key, SHAPES[name], jnp.float32)
    for key, name in zip(kv, NAMES, strict=True):
        drawn[f"v_{name}"] = jax.random.uniform(key, SHAPES[name], jnp.float32, 0.005, 0.015)
    return drawn


def matmul(a, w):
    return jnp.dot(a, w, preferred_element_type=jnp.float32).astype(jnp.bfloat16)


def normed(h):
    wide = h.astype(jnp.float32)
    scale = lax.rsqrt(jnp.mean(wide**2, -1, keepdims=True) + 1e-6)
    return (wide * scale).astype(jnp.bfloat16)


def layer(h, w):
    a = normed(h)
    gate = jnp.dot(a, w["w_gate"], preferred_element_type=jnp.float32)
    up = jnp.dot(a, w["w_up"], preferred_element_type=jnp.float32)
    return h + matmul((jax.nn.silu(gate) * up).astype(jnp.bfloat16), w["w_down"])


def adamw(w, m, v, g):
    m = 0.9 * m + 0.1 * g
    v = 0.95 * v + 0.05 * g * g
    step = m * lax.rsqrt(v + 1e-8) + 0.1 * w
    return (w - 0.02 * step).astype(jnp.bfloat16), m, v


def stack(weights, h):
    return lax.scan(lambda h, w: (layer(h, w), None), h, weights)[0]


def reference(x, dy, w_gate, w_up, w_down, m_w_gate, m_w_up, m_w_down, v_w_gate, v_w_up, v_w_down):
    weights = dict(zip(NAMES, (w_gate, w_up, w_down), strict=True))

    def take(so_far, sequence):
        h, by_y = sequence
        _, back = jax.vjp(lambda w: stack(w, h), weights)
        return jax.tree.map(lambda total, term: total + term.astype(jnp.float32), so_far, back(by_y)[0]), None

    none_yet = {name: jnp.zeros(w.shape, jnp.float32) for name, w in weights.items()}
    by_weights, _ = lax.scan(take, none_yet, (x, dy))
    gradients = [by_weights[name].astype(jnp.bfloat16).astype(jnp.float32) for name in NAMES]
    new = [
        adamw(w.astype(jnp.float32), m, v, g)
        for w, m, v, g in zip((w_gate, w_up, w_down), (m_w_gate, m_w_up, m_w_down), (v_w_gate, v_w_up, v_w_down), gradients, strict=True)
    ]
    return tuple(one[which] for which in range(3) for one in new)
```

```python
import functools
import jax, jax.numpy as jnp
from jax import lax
from jax.experimental import pallas as pl
from jax.experimental.pallas import tpu as pltpu
from jax.sharding import PartitionSpec as P

F32, BF16 = jnp.float32, jnp.bfloat16
TOK, D, W = 4096, 512, 512
T = 512
ANY = pl.BlockSpec(memory_space=pl.ANY)


def dot(a, b):
    return jnp.dot(a, b, preferred_element_type=F32)


def fwd_kernel(n, first, last, *refs):
    if first:
        a_h, p, out_h, a_v, y_v, sa, so = refs
    elif last:
        a_h, y_h, _, p, out_h, a_v, y_v, _, _, sa, sy, _, so = refs
    else:
        a_h, y_h, p, out_h, a_v, y_v, sa, sy, so = refs
    k = pl.program_id(0)

    def tile(ref, t):
        return ref.at[pl.ds(pl.multiple_of(t * T, T), T), :]

    def load(src, dst, sem, t):
        return pltpu.make_async_copy(tile(src, t), tile(dst, t), sem.at[t])

    @pl.when(k == 0)
    def _():
        for t in range(TOK // T):
            load(a_h, a_v, sa, t).start()
            if not first:
                load(y_h, y_v, sy, t).start()

    wg = p[:, 0, 0].reshape(D, W)
    wu = p[:, 0, 1].reshape(D, W)
    wd = p[:, 0, 2].reshape(W, D)

    @pl.loop(0, TOK // T)
    def _(t):
        @pl.when(k == 0)
        def _():
            load(a_h, a_v, sa, t).wait()
            if not first:
                load(y_h, y_v, sy, t).wait()
            else:
                tile(y_v, t)[...] = jnp.zeros((T, D), F32)

        a = tile(a_v, t)[...]
        gate = dot(a, wg)
        up = dot(a, wu)
        act = (gate * jax.nn.sigmoid(gate) * up).astype(BF16)
        tile(y_v, t)[...] += dot(act, wd)

        @pl.when(k == n - 1)
        def _():
            pltpu.make_async_copy(tile(y_v, t), tile(out_h, t), so.at[t]).start()

    @pl.when(k == n - 1)
    def _():
        for t in range(TOK // T):
            pltpu.make_async_copy(tile(y_v, t), tile(out_h, t), so.at[t]).wait()


def fwd(a, p, y=None):
    n = p.shape[1]
    first = y is None
    nt = TOK // T
    return pl.pallas_call(
        functools.partial(fwd_kernel, n, first, False),
        grid=(n,),
        out_shape=jax.ShapeDtypeStruct((TOK, D), F32),
        in_specs=[ANY] * (1 if first else 2) + [pl.BlockSpec((4, 1, 3, 128, 512), lambda k: (0, k, 0, 0, 0))],
        out_specs=ANY,
        scratch_shapes=[pltpu.VMEM((TOK, D), BF16), pltpu.VMEM((TOK, D), F32)] + [pltpu.SemaphoreType.DMA((nt,))] * (2 if first else 3),
        compiler_params=pltpu.CompilerParams(vmem_limit_bytes=60 << 20, dimension_semantics=("arbitrary",)),
        cost_estimate=pl.CostEstimate(flops=6 * TOK * D * W * n, bytes_accessed=n * 3 * (1 << 19) + (20 << 20), transcendentals=TOK * W * n),
        name="fwd",
    )(*((a,) if first else (a, y)), p)


def bwd_kernel(n, need, first, skip, *refs):
    refs = list(refs)[skip:]
    a_h, dy_h = refs[:2]; refs = refs[2:]
    if need and not first:
        da_h = refs.pop(0)
    p = refs.pop(0)
    g = refs.pop(0)
    if need:
        out_h = refs.pop(0)
    a_v, dy_v, aT, dyT, act_v, dg_v, du_v, wgT, wuT, wdT = refs[:10]; refs = refs[10:]
    if need:
        da_v = refs.pop(0)
    sa, sd = refs[:2]; refs = refs[2:]
    if need:
        sp, so = refs
    k = pl.program_id(0)
    nt = TOK // T

    def tile(ref, t):
        return ref.at[pl.ds(pl.multiple_of(t * T, T), T), :]

    def col(ref, t):
        return ref.at[:, pl.ds(pl.multiple_of(t * T, T), T)]

    def load(src, dst, sem, t):
        return pltpu.make_async_copy(tile(src, t), tile(dst, t), sem.at[t])

    @pl.when(k == 0)
    def _():
        for t in range(nt):
            load(a_h, a_v, sa, t).start()
            load(dy_h, dy_v, sd, t).start()
            if need and not first:
                load(da_h, da_v, sp, t).start()

    wg = p[:, 0, 0].reshape(D, W)
    wu = p[:, 0, 1].reshape(D, W)
    wd = p[:, 0, 2].reshape(W, D)
    wdT[...] = wd.T
    if need:
        wgT[...] = wg.T
        wuT[...] = wu.T

    @pl.loop(0, nt)
    def _(t):
        @pl.when(k == 0)
        def _():
            load(a_h, a_v, sa, t).wait()
            load(dy_h, dy_v, sd, t).wait()
            col(aT, t)[...] = tile(a_v, t)[...].T
            col(dyT, t)[...] = tile(dy_v, t)[...].T
            if need:
                if first:
                    tile(da_v, t)[...] = jnp.zeros((T, D), F32)
                else:
                    load(da_h, da_v, sp, t).wait()

        a = tile(a_v, t)[...]
        dy = tile(dy_v, t)[...]
        gate = dot(a, p[:, 0, 0].reshape(D, W))
        up = dot(a, p[:, 0, 1].reshape(D, W))
        dact = dot(dy, wdT[...]).astype(BF16).astype(F32)
        sig = jax.nn.sigmoid(gate)
        silu = gate * sig
        tile(act_v, t)[...] = (silu * up).astype(BF16)
        du = (dact * silu).astype(BF16)
        dg = (dact * up * (sig + silu * (1 - sig))).astype(BF16)
        tile(du_v, t)[...] = du
        tile(dg_v, t)[...] = dg
        if need:
            tile(da_v, t)[...] += dot(dg, wgT[...]) + dot(du, wuT[...])

            @pl.when(k == n - 1)
            def _():
                pltpu.make_async_copy(tile(da_v, t), tile(out_h, t), so.at[t]).start()

    g[:, 0, 0] = dot(aT[...], dg_v[...]).astype(BF16).reshape(4, 128, W)
    g[:, 0, 1] = dot(aT[...], du_v[...]).astype(BF16).reshape(4, 128, W)
    g[:, 0, 2] = dot(dyT[...], act_v[...]).astype(BF16).T.reshape(4, 128, D)

    if need:
        @pl.when(k == n - 1)
        def _():
            for t in range(nt):
                pltpu.make_async_copy(tile(da_v, t), tile(out_h, t), so.at[t]).wait()


def bwd(a, dy, p, da=None, need=True, deps=()):
    n = p.shape[1]
    first = da is None
    nt = TOK // T
    blk = pl.BlockSpec((4, 1, 3, 128, 512), lambda k: (0, k, 0, 0, 0))
    sem = pltpu.SemaphoreType.DMA((nt,))
    out = [jax.ShapeDtypeStruct((4, n, 3, 128, 512), BF16)] + ([jax.ShapeDtypeStruct((TOK, D), F32)] if need else [])
    args = tuple(deps) + (a, dy) + ((da,) if need and not first else ()) + (p,)
    big = lambda dt: pltpu.VMEM((TOK, D), dt)
    return pl.pallas_call(
        functools.partial(bwd_kernel, n, need, first, len(deps)),
        grid=(n,),
        out_shape=out,
        in_specs=[ANY] * (len(args) - 1) + [blk],
        out_specs=[blk] + ([ANY] if need else []),
        scratch_shapes=[big(BF16)] * 2 + [pltpu.VMEM((D, TOK), BF16)] * 2 + [big(BF16)] * 3 + [pltpu.VMEM((D, W), BF16)] * 3
        + ([big(F32)] if need else []) + [sem] * (4 if need else 2),
        compiler_params=pltpu.CompilerParams(vmem_limit_bytes=62 << 20, dimension_semantics=("arbitrary",)),
        cost_estimate=pl.CostEstimate(flops=2 * (8 if need else 6) * TOK * D * W * n, bytes_accessed=n * 6 * (1 << 19) + (20 << 20), transcendentals=TOK * W * n),
        name="bwd",
    )(*args)


CHUNKS = 4


def normed(h):
    wide = h.astype(F32)
    scale = lax.rsqrt(jnp.mean(wide**2, -1, keepdims=True) + 1e-6)
    return (wide * scale).astype(BF16)


def pack_kernel(*refs):
    gates, ups, down, out = refs[:4], refs[4:8], refs[8], refs[9]
    for k in range(4):
        for which, parts in ((0, gates), (1, ups)):
            for s in range(4):
                out[k, which, :, 128 * s : 128 * (s + 1)] = parts[s][0, :, 128 * k : 128 * (k + 1)]
        out[k, 2] = down[0, 128 * k : 128 * (k + 1), :]


def pack(l, j, w_gate, w_up, w_down):
    wide = [pl.BlockSpec((1, 128, 512), functools.partial(lambda s, i: (l, 0, 4 * s + j), s)) for s in range(4)]
    return pl.pallas_call(
        pack_kernel,
        grid=(1,),
        out_shape=jax.ShapeDtypeStruct((4, 3, 128, 512), BF16),
        in_specs=wide + wide + [pl.BlockSpec((1, 512, 512), lambda i: (l, j, 0))],
        out_specs=pl.BlockSpec((4, 3, 128, 512), lambda i: (0, 0, 0, 0)),
        cost_estimate=pl.CostEstimate(flops=1 << 21, bytes_accessed=3 << 20, transcendentals=0),
        name="pack",
    )(*[w_gate] * 4, *[w_up] * 4, w_down)


def adamw(w, m, v, g):
    m = 0.9 * m + 0.1 * g
    v = 0.95 * v + 0.05 * g * g
    step = m * lax.rsqrt(v + 1e-8) + 0.1 * w
    return (w - 0.02 * step).astype(BF16), m, v


def adam_kernel(*refs):
    gs, gr, w, m, v = (refs[3 * i : 3 * i + 3] for i in range(5))
    outs = refs[-10:-1]
    refs[-1][...] = jnp.zeros((8, 128), F32)
    for which in range(3):
        g = (gs[which][...].astype(F32) + gr[which][...].astype(F32)).astype(BF16).astype(F32)
        for k in range(4 if which < 2 else 1):
            c = slice(128 * k, 128 * (k + 1)) if which < 2 else slice(0, 512)
            new = adamw(w[which][0, :, c].astype(F32), m[which][0, :, c], v[which][0, :, c], g[k, 0])
            for i in range(3):
                outs[3 * i + which][0, :, c] = new[i]


def adam(l, j, gs, gr, weights, m, v, before):
    cols = [pl.BlockSpec((4, 1, 128, 128), functools.partial(lambda which, i: (0, which, 0, i), which)) for which in range(2)]
    cols.append(pl.BlockSpec((1, 1, 128, 512), lambda i: (i, 2, 0, 0)))
    own = [pl.BlockSpec((1, 128, 512), lambda i: (l, 0, 4 * i + j))] * 2 + [pl.BlockSpec((1, 128, 512), lambda i: (l, 4 * j + i, 0))]
    shapes = [jax.ShapeDtypeStruct(w.shape, dt) for dt in (BF16, F32, F32) for w in weights]
    shapes.append(jax.ShapeDtypeStruct((8, 128), F32))
    before = list(before or [])
    return pl.pallas_call(
        adam_kernel,
        grid=(4,),
        out_shape=shapes,
        in_specs=cols * 2 + own * 3 + [ANY] * len(before),
        out_specs=own * 3 + [pl.BlockSpec((8, 128), lambda i: (0, 0))],
        input_output_aliases={15 + i: i for i in range(len(before))},
        cost_estimate=pl.CostEstimate(flops=10 * 3 * 4 * 128 * 512, bytes_accessed=18 << 20, transcendentals=3 * 4 * 128 * 512),
        name="adam",
    )(*[gs] * 3, *[gr] * 3, *weights, *m, *v, *before)


def solution(mesh):
    pairs = [(0, 1), (1, 0)]

    def step(x, dy, *arrays):
        weights, m, v = (arrays[i : i + 3] for i in (0, 3, 6))
        x, dy = x[0], dy[0]
        full = [[lax.all_gather(pack(l, j, *weights), "s", axis=0) for j in range(CHUNKS)] for l in range(2)]
        a0 = normed(x)
        y = None
        for j in range(CHUNKS):
            y = fwd(a0, full[0][j], y)
        h1 = x + y.astype(BF16)
        a1, back = jax.vjp(normed, h1)
        order = [(1, j) for j in range(CHUNKS)] + [(0, j) for j in range(CHUNKS)]
        ours, theirs, out, marks, da = [], [], None, [], None

        def settle(i):
            nonlocal out
            *out, mark = adam(*order[i], ours[i], theirs[i], weights, m, v, out)
            marks.append(mark)

        for i, (l, j) in enumerate(order):
            deps = []
            if i >= 3:
                settle(i - 3)
                deps = [ours[i - 2], marks[i - 3]]
            if (l, j) == (0, 0):
                dh = dy + back(da.astype(BF16))[0]
            if i >= 2:
                theirs.append(lax.ppermute(ours[i - 2], "r", pairs))
            if l == 1:
                term, da = bwd(a1, dy, full[1][j], da, deps=deps)
            else:
                term = bwd(a0, dh, full[0][j], need=False, deps=deps)[0]
            ours.append(lax.psum_scatter(term, "s", scatter_dimension=0, tiled=True)[0])
        theirs += [lax.ppermute(one, "r", pairs) for one in ours[-2:]]
        for i in range(len(order) - 3, len(order)):
            settle(i)
        return tuple(out)

    states, cut = P(("rep", "r", "s"), None, None), P(None, "s", None)
    return jax.shard_map(
        step,
        mesh=mesh,
        in_specs=(states, states) + (cut,) * 9,
        out_specs=(P("rep", "s", None),) * 9,
        check_vma=False,
    )
```

```python
import functools
import jax, jax.numpy as jnp
from jax import lax
from jax.experimental import pallas as pl
from jax.experimental.pallas import tpu as pltpu
from jax.sharding import PartitionSpec as P

F32, BF16 = jnp.float32, jnp.bfloat16
TOK, D, W = 4096, 512, 512
T = 512
NT = TOK // T
ROWS = 32
ANY = pl.BlockSpec(memory_space=pl.ANY)
STRIP = pl.BlockSpec((4, 1, 3, 128, 512), lambda k: (0, k, 0, 0, 0))


def dot(a, b):
    return jnp.dot(a, b, preferred_element_type=F32)


def tile(ref, t):
    return ref.at[pl.ds(pl.multiple_of(t * T, T), T), :]


def copies(src, dst, sem, t):
    return pltpu.make_async_copy(tile(src, t), tile(dst, t), sem.at[t])


def pipelined(head, tail, before, after):
    before(0, 1)
    head(0, 0)

    @pl.loop(0, NT // 2 - 1)
    def _(i):
        before(2 * i + 1, 2)
        head(2 * i + 1, 1)
        tail(2 * i, 0)
        head(2 * i + 2, 0)
        tail(2 * i + 1, 1)
        after(2 * i, 2)

    before(NT - 1, 1)
    head(NT - 1, 1)
    tail(NT - 2, 0)
    tail(NT - 1, 1)


def fwd_kernel(n, first, *refs):
    refs = list(refs)
    a_h = refs.pop(0)
    y_h = None if first else refs.pop(0)
    p, out_h, a_v, y_v, g0, u0, g1, u1, act_s, sa, sy, so = refs
    k = pl.program_id(0)
    gate_s, up_s = (g0, g1), (u0, u1)

    @pl.when(k == 0)
    def _():
        for t in range(NT):
            copies(a_h, a_v, sa, t).start()
            if not first:
                copies(y_h, y_v, sy, t).start()

    def before(t, count):
        @pl.when(k == 0)
        def _():
            for i in range(count):
                copies(a_h, a_v, sa, t + i).wait()
                if not first:
                    copies(y_h, y_v, sy, t + i).wait()

    def head(t, slot):
        a = tile(a_v, t)[...]
        gate_s[slot][...] = dot(a, p[:, 0, 0].reshape(D, W))
        up_s[slot][...] = dot(a, p[:, 0, 1].reshape(D, W))

    def tail(t, slot):
        for r in range(0, T, ROWS):
            gate = gate_s[slot][r : r + ROWS]
            act_s[r : r + ROWS] = (gate * jax.nn.sigmoid(gate) * up_s[slot][r : r + ROWS]).astype(BF16)
        old = tile(y_v, t)[...]
        if first:
            old = jnp.where(k == 0, 0.0, old)
        tile(y_v, t)[...] = old + dot(act_s[...], p[:, 0, 2].reshape(W, D))

    def after(t, count):
        @pl.when(k == n - 1)
        def _():
            for i in range(count):
                copies(y_v, out_h, so, t + i).start()

    pipelined(head, tail, before, after)
    after(NT - 2, 2)

    @pl.when(k == n - 1)
    def _():
        for t in range(NT):
            copies(y_v, out_h, so, t).wait()


def fwd(a, p, y=None):
    n = p.shape[1]
    first = y is None
    sem = pltpu.SemaphoreType.DMA((NT,))
    return pl.pallas_call(
        functools.partial(fwd_kernel, n, first),
        grid=(n,),
        out_shape=jax.ShapeDtypeStruct((TOK, D), F32),
        in_specs=[ANY] * (1 if first else 2) + [STRIP],
        out_specs=ANY,
        scratch_shapes=[pltpu.VMEM((TOK, D), BF16), pltpu.VMEM((TOK, D), F32)] + [pltpu.VMEM((T, W), F32)] * 4 + [pltpu.VMEM((T, W), BF16)] + [sem] * 3,
        compiler_params=pltpu.CompilerParams(vmem_limit_bytes=60 << 20, dimension_semantics=("arbitrary",)),
        cost_estimate=pl.CostEstimate(flops=6 * TOK * D * W * n, bytes_accessed=n * 3 * (1 << 19) + (20 << 20), transcendentals=TOK * W * n),
        name="fwd",
    )(*((a,) if first else (a, y)), p)


def adamw(w, m, v, g):
    m = 0.9 * m + 0.1 * g
    v = 0.95 * v + 0.05 * g * g
    step = m * lax.rsqrt(v + 1e-8) + 0.1 * w
    return (w - 0.02 * step).astype(BF16), m, v


def adam_step(ins, outs):
    gs, gr, w, m, v = (ins[3 * i : 3 * i + 3] for i in range(5))
    for which in range(3):
        g = (gs[which][...].astype(F32) + gr[which][...].astype(F32)).astype(BF16).astype(F32)
        for k in range(4 if which < 2 else 1):
            c = slice(128 * k, 128 * (k + 1)) if which < 2 else slice(0, 512)
            new = adamw(w[which][0, :, c].astype(F32), m[which][0, :, c], v[which][0, :, c], g[k, 0])
            for i in range(3):
                outs[3 * i + which][0, :, c] = new[i]


def adam_specs(l, j):
    cols = [pl.BlockSpec((4, 1, 128, 128), functools.partial(lambda which, i: (0, which, 0, i), which)) for which in range(2)]
    cols.append(pl.BlockSpec((1, 1, 128, 512), lambda i: (i, 2, 0, 0)))
    own = [pl.BlockSpec((1, 128, 512), lambda i: (l, 0, 4 * i + j))] * 2 + [pl.BlockSpec((1, 128, 512), lambda i: (l, 4 * j + i, 0))]
    return cols * 2 + own * 3, own * 3


def bwd_kernel(n, need, first, state, skip, *refs):
    refs = list(refs)
    take = lambda count: [refs.pop(0) for _ in range(count)]
    take(skip)
    ad_in = take(15) if state else []
    a_h, dy_h, aT_h, dyT_h = take(4)
    da_h = take(1)[0] if need and not first else None
    p = refs.pop(0)
    g = refs.pop(0)
    out_h = refs.pop(0) if need else None
    ad_out = take(9) if state else []
    a_v, dy_v, aT, dyT, act_v, dgu_v, wT, wdT = take(8)
    gate_s, up_s, dact_s = take(2), take(2), take(2)
    da_v = refs.pop(0) if need else None
    sa, sd, st = take(3)
    sp, so = take(2) if need else (None, None)
    k = pl.program_id(0)

    def turned(which):
        return pltpu.make_async_copy((aT_h, dyT_h)[which], (aT, dyT)[which], st.at[which])

    @pl.when(k == 0)
    def _():
        for t in range(NT):
            copies(a_h, a_v, sa, t).start()
            copies(dy_h, dy_v, sd, t).start()
            if need and not first:
                copies(da_h, da_v, sp, t).start()
        for which in range(2):
            turned(which).start()

    def before(t, count):
        @pl.when(k == 0)
        def _():
            for i in range(count):
                copies(a_h, a_v, sa, t + i).wait()
                copies(dy_h, dy_v, sd, t + i).wait()
                if need and not first:
                    copies(da_h, da_v, sp, t + i).wait()

    def head(t, slot):
        a = tile(a_v, t)[...]
        gate_s[slot][...] = dot(a, p[:, 0, 0].reshape(D, W))
        up_s[slot][...] = dot(a, p[:, 0, 1].reshape(D, W))
        dact_s[slot][...] = dot(tile(dy_v, t)[...], wdT[...]).astype(BF16)

    def tail(t, slot):
        for r in range(0, T, ROWS):
            rows = slice(r, r + ROWS)
            here = pl.ds(pl.multiple_of(t * T + r, ROWS), ROWS)
            gate, up, dact = gate_s[slot][rows], up_s[slot][rows], dact_s[slot][rows].astype(F32)
            sig = jax.nn.sigmoid(gate)
            silu = gate * sig
            act_v[here] = (silu * up).astype(BF16)
            dgu_v[here, W:] = (dact * silu).astype(BF16)
            dgu_v[here, :W] = (dact * up * (sig + silu * (1 - sig))).astype(BF16)
        if need:
            old = tile(da_v, t)[...]
            if first:
                old = jnp.where(k == 0, 0.0, old)
            tile(da_v, t)[...] = old + dot(tile(dgu_v, t)[...], wT[...])

    def after(t, count):
        if need:
            @pl.when(k == n - 1)
            def _():
                for i in range(count):
                    copies(da_v, out_h, so, t + i).start()

    wdT[...] = p[:, 0, 2].reshape(W, D).T
    if need:
        wT[:W] = p[:, 0, 0].reshape(D, W).T
        wT[W:] = p[:, 0, 1].reshape(D, W).T
    pipelined(head, tail, before, after)
    after(NT - 2, 2)

    @pl.when(k == 0)
    def _():
        for which in range(2):
            turned(which).wait()

    for which in range(2):
        g[:, 0, which] = dot(aT[...], dgu_v[:, W * which : W * (which + 1)]).astype(BF16).reshape(4, 128, W)
    g[:, 0, 2] = dot(dyT[...], act_v[...]).astype(BF16).T.reshape(4, 128, D)
    if state:
        adam_step(ad_in, ad_out)

    if need:
        @pl.when(k == n - 1)
        def _():
            for t in range(NT):
                copies(da_v, out_h, so, t).wait()


def bwd(a, dy, aT, dyT, p, da=None, need=True, deps=(), state=None):
    n = p.shape[1]
    first = da is None
    sem = pltpu.SemaphoreType.DMA((NT,))
    args = list(deps)
    specs = [ANY] * len(args)
    out_shapes = [jax.ShapeDtypeStruct((4, n, 3, 128, 512), BF16)]
    out_specs = [STRIP]
    if need:
        out_shapes.append(jax.ShapeDtypeStruct((TOK, D), F32))
        out_specs.append(ANY)
    aliases = {}
    if state:
        l, j, gs, gr, weights, m, v, before = state
        before = list(before or [])
        aliases = {len(args) + i: len(out_shapes) + i for i in range(len(before))}
        args += before
        specs += [ANY] * len(before)
    skip = len(args)
    if state:
        ins, outs = adam_specs(l, j)
        args += [gs] * 3 + [gr] * 3 + [*weights, *m, *v]
        specs += ins
        out_shapes += [jax.ShapeDtypeStruct(w.shape, dt) for dt in (BF16, F32, F32) for w in weights]
        out_specs += outs
    rest = [a, dy, aT, dyT] + ([da] if need and not first else [])
    args += rest + [p]
    specs += [ANY] * len(rest) + [STRIP]
    big = lambda dt: pltpu.VMEM((TOK, D), dt)
    return pl.pallas_call(
        functools.partial(bwd_kernel, n, need, first, bool(state), skip),
        grid=(n,),
        out_shape=out_shapes,
        in_specs=specs,
        out_specs=out_specs,
        scratch_shapes=[big(BF16)] * 2 + [pltpu.VMEM((D, TOK), BF16)] * 2 + [big(BF16), pltpu.VMEM((TOK, 2 * W), BF16), pltpu.VMEM((2 * W, D), BF16), pltpu.VMEM((D, W), BF16)]
        + [pltpu.VMEM((T, W), F32)] * 4 + [pltpu.VMEM((T, W), BF16)] * 2
        + ([big(F32)] if need else []) + [sem] * 2 + [pltpu.SemaphoreType.DMA((2,))] + ([sem] * 2 if need else []),
        input_output_aliases=aliases,
        compiler_params=pltpu.CompilerParams(vmem_limit_bytes=63 << 20, dimension_semantics=("arbitrary",)),
        cost_estimate=pl.CostEstimate(flops=2 * (8 if need else 6) * TOK * D * W * n, bytes_accessed=n * 6 * (1 << 19) + (20 << 20), transcendentals=TOK * W * n),
        name="bwd",
    )(*args)


def normed(h):
    wide = h.astype(F32)
    scale = lax.rsqrt(jnp.mean(wide**2, -1, keepdims=True) + 1e-6)
    return (wide * scale).astype(BF16)


def rowwise(body, ins, outs):
    spec = lambda one: pl.BlockSpec((T, D), lambda t: (t, 0)) if one.shape[0] == TOK else pl.BlockSpec((D, T), lambda t: (0, t))
    return pl.pallas_call(
        body,
        grid=(NT,),
        out_shape=outs,
        in_specs=[spec(one) for one in ins],
        out_specs=[spec(one) for one in outs],
        cost_estimate=pl.CostEstimate(flops=20 * TOK * D, bytes_accessed=24 << 20, transcendentals=TOK),
    )(*ins)


ROW, COL = jax.ShapeDtypeStruct((TOK, D), BF16), jax.ShapeDtypeStruct((D, TOK), BF16)


def start_kernel(x, dy, a, aT, dyT):
    a[...] = normed(x[...])
    aT[...] = a[...].T
    dyT[...] = dy[...].T


def middle_kernel(x, y, h, a, aT):
    h[...] = (x[...].astype(F32) + y[...].astype(BF16).astype(F32)).astype(BF16)
    a[...] = normed(h[...])
    aT[...] = a[...].T


def back_kernel(h, dy, da, dh, dhT):
    wide = h[...].astype(F32)
    scale = lax.rsqrt(jnp.mean(wide**2, -1, keepdims=True) + 1e-6)
    by_a = da[...].astype(BF16).astype(F32)
    by_h = by_a * scale - wide * (scale * scale * scale * jnp.mean(by_a * wide, -1, keepdims=True))
    dh[...] = (dy[...].astype(F32) + by_h.astype(BF16).astype(F32)).astype(BF16)
    dhT[...] = dh[...].T


CHUNKS = 4


def pack_kernel(*refs):
    gates, ups, down, out = refs[:4], refs[4:8], refs[8], refs[9]
    for k in range(4):
        for which, parts in ((0, gates), (1, ups)):
            for s in range(4):
                out[k, which, :, 128 * s : 128 * (s + 1)] = parts[s][0, :, 128 * k : 128 * (k + 1)]
        out[k, 2] = down[0, 128 * k : 128 * (k + 1), :]


def pack(l, j, w_gate, w_up, w_down):
    wide = [pl.BlockSpec((1, 128, 512), functools.partial(lambda s, i: (l, 0, 4 * s + j), s)) for s in range(4)]
    return pl.pallas_call(
        pack_kernel,
        grid=(1,),
        out_shape=jax.ShapeDtypeStruct((4, 3, 128, 512), BF16),
        in_specs=wide + wide + [pl.BlockSpec((1, 512, 512), lambda i: (l, j, 0))],
        out_specs=pl.BlockSpec((4, 3, 128, 512), lambda i: (0, 0, 0, 0)),
        cost_estimate=pl.CostEstimate(flops=1 << 21, bytes_accessed=3 << 20, transcendentals=0),
        name="pack",
    )(*[w_gate] * 4, *[w_up] * 4, w_down)


def adam_kernel(skip, *refs):
    adam_step(refs[skip : skip + 15], refs[skip + 15 : skip + 24])


def adam(l, j, gs, gr, weights, m, v, before):
    ins, outs = adam_specs(l, j)
    shapes = [jax.ShapeDtypeStruct(w.shape, dt) for dt in (BF16, F32, F32) for w in weights]
    before = list(before or [])
    return pl.pallas_call(
        functools.partial(adam_kernel, len(before)),
        grid=(4,),
        out_shape=shapes,
        in_specs=[ANY] * len(before) + ins,
        out_specs=outs,
        input_output_aliases={i: i for i in range(len(before))},
        cost_estimate=pl.CostEstimate(flops=10 * 3 * 4 * 128 * 512, bytes_accessed=18 << 20, transcendentals=3 * 4 * 128 * 512),
        name="adam",
    )(*before, *[gs] * 3, *[gr] * 3, *weights, *m, *v)


def solution(mesh):
    pairs = [(0, 1), (1, 0)]

    def step(x, dy, *arrays):
        weights, m, v = (arrays[i : i + 3] for i in (0, 3, 6))
        x, dy = x[0], dy[0]
        full = [[lax.all_gather(pack(l, j, *weights), "s", axis=0) for j in range(CHUNKS)] for l in range(2)]
        a0, a0T, dyT = rowwise(start_kernel, [x, dy], [ROW, COL, COL])
        y = None
        for j in range(CHUNKS):
            y = fwd(a0, full[0][j], y)
        h1, a1, a1T = rowwise(middle_kernel, [x, y], [ROW, ROW, COL])
        order = [(1, j) for j in range(CHUNKS)] + [(0, j) for j in range(CHUNKS)]
        ours, theirs, out, da = [], [], None, None
        for i, (l, j) in enumerate(order):
            deps, state = [], None
            if i >= 3:
                deps = [ours[i - 2]]
            if i >= 4:
                state = (*order[i - 4], ours[i - 4], theirs[i - 4], weights, m, v, out)
            if (l, j) == (0, 0):
                dh, dhT = rowwise(back_kernel, [h1, dy, da], [ROW, COL])
            if i >= 2:
                theirs.append(lax.ppermute(ours[i - 2], "r", pairs))
            if l == 1:
                term, da, *new = bwd(a1, dy, a1T, dyT, full[1][j], da, deps=deps, state=state)
            else:
                term, *new = bwd(a0, dh, a0T, dhT, full[0][j], need=False, deps=deps, state=state)
            if state:
                out = new
            ours.append(lax.psum_scatter(term, "s", scatter_dimension=0, tiled=True)[0])
        last = len(order) - 1
        theirs.append(lax.ppermute(ours[last - 1], "r", pairs))
        for i in range(last - 3, last):
            out = adam(*order[i], ours[i], theirs[i], weights, m, v, out)
        theirs.append(lax.ppermute(ours[last], "r", pairs))
        out = adam(*order[last], ours[last], theirs[last], weights, m, v, out)
        return tuple(out)

    states, cut = P(("rep", "r", "s"), None, None), P(None, "s", None)
    return jax.shard_map(
        step,
        mesh=mesh,
        in_specs=(states, states) + (cut,) * 9,
        out_specs=(P("rep", "s", None),) * 9,
        check_vma=False,
    )
```

```python
import functools
import jax, jax.numpy as jnp
from jax import lax
from jax.experimental import pallas as pl
from jax.experimental.pallas import tpu as pltpu
from jax.sharding import PartitionSpec as P

F32, BF16 = jnp.float32, jnp.bfloat16
TOK, D, W = 4096, 512, 512
T = 512
NT = TOK // T
ROWS = 32
ANY = pl.BlockSpec(memory_space=pl.ANY)
STRIP = pl.BlockSpec((4, 1, 3, 128, 512), lambda k: (0, k, 0, 0, 0))


def dot(a, b):
    return jnp.dot(a, b, preferred_element_type=F32)


def tile(ref, t):
    return ref.at[pl.ds(pl.multiple_of(t * T, T), T), :]


def copies(src, dst, sem, t):
    return pltpu.make_async_copy(tile(src, t), tile(dst, t), sem.at[t])


def pipelined(head, tail, before, after):
    before(0, 1)
    head(0, 0)

    @pl.loop(0, NT // 2 - 1)
    def _(i):
        before(2 * i + 1, 2)
        head(2 * i + 1, 1)
        tail(2 * i, 0)
        head(2 * i + 2, 0)
        tail(2 * i + 1, 1)
        after(2 * i, 2)

    before(NT - 1, 1)
    head(NT - 1, 1)
    tail(NT - 2, 0)
    tail(NT - 1, 1)


def adamw(w, m, v, g):
    m = 0.9 * m + 0.1 * g
    v = 0.95 * v + 0.05 * g * g
    step = m * lax.rsqrt(v + 1e-8) + 0.1 * w
    return (w - 0.02 * step).astype(BF16), m, v


def adam_step(ins, outs):
    gs, gr, w, m, v = (ins[3 * i : 3 * i + 3] for i in range(5))
    for which in range(3):
        g = (gs[which][...].astype(F32) + gr[which][...].astype(F32)).astype(BF16).astype(F32)
        for k in range(4 if which < 2 else 1):
            c = slice(128 * k, 128 * (k + 1)) if which < 2 else slice(0, 512)
            new = adamw(w[which][0, :, c].astype(F32), m[which][0, :, c], v[which][0, :, c], g[k, 0])
            for i in range(3):
                outs[3 * i + which][0, :, c] = new[i]


def adam_specs(l, j):
    cols = [pl.BlockSpec((4, 1, 128, 128), functools.partial(lambda which, i: (0, which, 0, i), which)) for which in range(2)]
    cols.append(pl.BlockSpec((1, 1, 128, 512), lambda i: (i, 2, 0, 0)))
    own = [pl.BlockSpec((1, 128, 512), lambda i: (l, 0, 4 * i + j))] * 2 + [pl.BlockSpec((1, 128, 512), lambda i: (l, 4 * j + i, 0))]
    return cols * 2 + own * 3, own * 3


def bwd_kernel(n, need, first, state, skip, *refs):
    refs = list(refs)
    take = lambda count: [refs.pop(0) for _ in range(count)]
    take(skip)
    ad_in = take(15) if state else []
    a_h, dy_h, aT_h, dyT_h = take(4)
    da_h = take(1)[0] if need and not first else None
    p = refs.pop(0)
    g = refs.pop(0)
    out_h = refs.pop(0) if need else None
    ad_out = take(9) if state else []
    a_v, dy_v, aT, dyT, act_v, dgu_v, wT, wdT = take(8)
    gate_s, up_s, dact_s = take(2), take(2), take(2)
    da_v = refs.pop(0) if need else None
    sa, sd, st = take(3)
    sp, so = take(2) if need else (None, None)
    k = pl.program_id(0)

    def turned(which):
        return pltpu.make_async_copy((aT_h, dyT_h)[which], (aT, dyT)[which], st.at[which])

    @pl.when(k == 0)
    def _():
        for t in range(NT):
            copies(a_h, a_v, sa, t).start()
            copies(dy_h, dy_v, sd, t).start()
            if need and not first:
                copies(da_h, da_v, sp, t).start()
        for which in range(2):
            turned(which).start()

    def before(t, count):
        @pl.when(k == 0)
        def _():
            for i in range(count):
                copies(a_h, a_v, sa, t + i).wait()
                copies(dy_h, dy_v, sd, t + i).wait()
                if need and not first:
                    copies(da_h, da_v, sp, t + i).wait()

    def head(t, slot):
        a = tile(a_v, t)[...]
        gate_s[slot][...] = dot(a, p[:, 0, 0].reshape(D, W))
        up_s[slot][...] = dot(a, p[:, 0, 1].reshape(D, W))
        dact_s[slot][...] = dot(tile(dy_v, t)[...], wdT[...]).astype(BF16)

    def tail(t, slot):
        for r in range(0, T, ROWS):
            rows = slice(r, r + ROWS)
            here = pl.ds(pl.multiple_of(t * T + r, ROWS), ROWS)
            gate, up, dact = gate_s[slot][rows], up_s[slot][rows], dact_s[slot][rows].astype(F32)
            sig = jax.nn.sigmoid(gate)
            silu = gate * sig
            act_v[here] = (silu * up).astype(BF16)
            dgu_v[here, W:] = (dact * silu).astype(BF16)
            dgu_v[here, :W] = (dact * up * (sig + silu * (1 - sig))).astype(BF16)
        if need:
            old = tile(da_v, t)[...]
            if first:
                old = jnp.where(k == 0, 0.0, old)
            tile(da_v, t)[...] = old + dot(tile(dgu_v, t)[...], wT[...])

    def after(t, count):
        if need:
            @pl.when(k == n - 1)
            def _():
                for i in range(count):
                    copies(da_v, out_h, so, t + i).start()

    wdT[...] = p[:, 0, 2].reshape(W, D).T
    if need:
        wT[:W] = p[:, 0, 0].reshape(D, W).T
        wT[W:] = p[:, 0, 1].reshape(D, W).T
    pipelined(head, tail, before, after)
    after(NT - 2, 2)

    @pl.when(k == 0)
    def _():
        for which in range(2):
            turned(which).wait()

    for which in range(2):
        g[:, 0, which] = dot(aT[...], dgu_v[:, W * which : W * (which + 1)]).astype(BF16).reshape(4, 128, W)
    g[:, 0, 2] = dot(dyT[...], act_v[...]).astype(BF16).T.reshape(4, 128, D)
    if state:
        adam_step(ad_in, ad_out)

    if need:
        @pl.when(k == n - 1)
        def _():
            for t in range(NT):
                copies(da_v, out_h, so, t).wait()


def bwd(a, dy, aT, dyT, p, at, da=None, need=True, deps=(), state=None):
    n = 4
    first = da is None
    sem = pltpu.SemaphoreType.DMA((NT,))
    args = list(deps)
    specs = [ANY] * len(args)
    out_shapes = [jax.ShapeDtypeStruct((4, n, 3, 128, 512), BF16)]
    out_specs = [STRIP]
    if need:
        out_shapes.append(jax.ShapeDtypeStruct((TOK, D), F32))
        out_specs.append(ANY)
    aliases = {}
    if state:
        l, j, gs, gr, weights, m, v, before = state
        before = list(before or [])
        aliases = {len(args) + i: len(out_shapes) + i for i in range(len(before))}
        args += before
        specs += [ANY] * len(before)
    skip = len(args)
    if state:
        ins, outs = adam_specs(l, j)
        args += [gs] * 3 + [gr] * 3 + [*weights, *m, *v]
        specs += ins
        out_shapes += [jax.ShapeDtypeStruct(w.shape, dt) for dt in (BF16, F32, F32) for w in weights]
        out_specs += outs
    rest = [a, dy, aT, dyT] + ([da] if need and not first else [])
    args += rest + [p]
    specs += [ANY] * len(rest) + [pl.BlockSpec((4, 1, 3, 128, 512), lambda k: (0, at + k, 0, 0, 0))]
    big = lambda dt: pltpu.VMEM((TOK, D), dt)
    return pl.pallas_call(
        functools.partial(bwd_kernel, n, need, first, bool(state), skip),
        grid=(n,),
        out_shape=out_shapes,
        in_specs=specs,
        out_specs=out_specs,
        scratch_shapes=[big(BF16)] * 2 + [pltpu.VMEM((D, TOK), BF16)] * 2 + [big(BF16), pltpu.VMEM((TOK, 2 * W), BF16), pltpu.VMEM((2 * W, D), BF16), pltpu.VMEM((D, W), BF16)]
        + [pltpu.VMEM((T, W), F32)] * 4 + [pltpu.VMEM((T, W), BF16)] * 2
        + ([big(F32)] if need else []) + [sem] * 2 + [pltpu.SemaphoreType.DMA((2,))] + ([sem] * 2 if need else []),
        input_output_aliases=aliases,
        compiler_params=pltpu.CompilerParams(vmem_limit_bytes=63 << 20, dimension_semantics=("arbitrary",)),
        cost_estimate=pl.CostEstimate(flops=2 * (8 if need else 6) * TOK * D * W * n, bytes_accessed=n * 6 * (1 << 19) + (20 << 20), transcendentals=TOK * W * n),
        name="bwd",
    )(*args)


def normed(h):
    wide = h.astype(F32)
    scale = lax.rsqrt(jnp.mean(wide**2, -1, keepdims=True) + 1e-6)
    return (wide * scale).astype(BF16)


def rowwise(body, ins, outs):
    spec = lambda one: pl.BlockSpec((T, D), lambda t: (t, 0)) if one.shape[0] == TOK else pl.BlockSpec((D, T), lambda t: (0, t))
    return pl.pallas_call(
        body,
        grid=(NT,),
        out_shape=outs,
        in_specs=[spec(one) for one in ins],
        out_specs=[spec(one) for one in outs],
        cost_estimate=pl.CostEstimate(flops=20 * TOK * D, bytes_accessed=24 << 20, transcendentals=TOK),
    )(*ins)


ROW, COL = jax.ShapeDtypeStruct((TOK, D), BF16), jax.ShapeDtypeStruct((D, TOK), BF16)


def middle_kernel(x, y, dy, h, a, aT, dyT):
    h[...] = (x[...].astype(F32) + y[...].astype(BF16).astype(F32)).astype(BF16)
    a[...] = normed(h[...])
    aT[...] = a[...].T
    dyT[...] = dy[...].T


def back_kernel(h, dy, da, a, dh, dhT, aT):
    wide = h[...].astype(F32)
    scale = lax.rsqrt(jnp.mean(wide**2, -1, keepdims=True) + 1e-6)
    by_a = da[...].astype(BF16).astype(F32)
    by_h = by_a * scale - wide * (scale * scale * scale * jnp.mean(by_a * wide, -1, keepdims=True))
    dh[...] = (dy[...].astype(F32) + by_h.astype(BF16).astype(F32)).astype(BF16)
    dhT[...] = dh[...].T
    aT[...] = a[...].T


STRIPS = 16


def pack_kernel(base, *refs):
    gates, ups, down = refs[:4], refs[4:8], refs[8]
    outs = refs[9:]
    for i, (lo, hi) in enumerate(base):
        @pl.when((pl.program_id(0) >= lo) & (pl.program_id(0) < hi))
        def _(out=outs[i]):
            for k in range(4):
                for which, parts in ((0, gates), (1, ups)):
                    for s in range(4):
                        out[k, which, :, 128 * s : 128 * (s + 1)] = parts[s][0, :, 128 * k : 128 * (k + 1)]
                out[k, 2] = down[0, 128 * k : 128 * (k + 1), :]


def pack(l, base, w_gate, w_up, w_down):
    wide = [pl.BlockSpec((1, 128, 512), functools.partial(lambda s, j: (l, 0, 4 * s + j), s)) for s in range(4)]
    return pl.pallas_call(
        functools.partial(pack_kernel, base),
        grid=(4,),
        out_shape=[jax.ShapeDtypeStruct((4 * (hi - lo), 3, 128, 512), BF16) for lo, hi in base],
        in_specs=wide + wide + [pl.BlockSpec((1, 512, 512), lambda j: (l, j, 0))],
        out_specs=[pl.BlockSpec((4, 3, 128, 512), functools.partial(lambda lo, hi, j: (jnp.clip(j - lo, 0, hi - lo - 1), 0, 0, 0), lo, hi)) for lo, hi in base],
        cost_estimate=pl.CostEstimate(flops=1 << 21, bytes_accessed=12 << 20, transcendentals=0),
        name="pack",
    )(*[w_gate] * 4, *[w_up] * 4, w_down)


def gather_kernel(x_h, pk, full_h, a_h, y_h, full, a_v, y_v, g0, u0, g1, u1, act_s, *sems):
    load, own, x_send, x_recv, y_send, y_recv, own_send, own_recv, on_send, on_recv, put, a_out, y_out = sems
    gate_s, up_s = (g0, g1), (u0, u1)
    s, r = lax.axis_index("s"), lax.axis_index("r")
    by_x, by_core = lax.rem(s + 2, 4), s + 1 - 2 * lax.rem(s, 2)
    far = lax.rem(by_core + 2, 4)

    def remote(src, block, k, send, recv, where):
        return pltpu.make_async_remote_copy(
            src_ref=src, dst_ref=full.at[block, k], send_sem=send.at[k], recv_sem=recv.at[k],
            device_id=where, device_id_type=pl.DeviceIdType.MESH,
        )

    def strip(b):
        odd, first, last = lax.rem(b, 2), (15 - b) // 15, b // 15
        return odd * (b + 1 + r) + (1 - odd) * (b - 1 - r) + (first - last) * (1 + 2 * r), odd * (1 - last) + first

    def from_x(block, k):
        return remote(pk.at[k], block, k, x_send, x_recv, {"s": by_x})

    def from_y(block, k):
        return remote(full.at[block, k], block, k, y_send, y_recv, {"r": 1 - r})

    def from_core(block, k):
        return remote(pk.at[k], block, k, own_send, own_recv, {"s": by_core})

    def handed_on(block, k):
        return remote(full.at[block, k], block, k, on_send, on_recv, {"s": by_core})

    def mine(k):
        return pltpu.make_async_copy(pk.at[k], full.at[s, k], own.at[k])

    def kept(k):
        return pltpu.make_async_copy(full.at[:, k], full_h.at[:, k], put.at[k])

    for t in range(NT):
        copies(x_h, a_v, load, t).start()
    barrier = pltpu.get_barrier_semaphore()
    for where in ({"s": by_x}, {"s": by_core}, {"r": 1 - r}):
        pl.semaphore_signal(barrier, inc=1, device_id=where, device_id_type=pl.DeviceIdType.MESH)
    pl.semaphore_wait(barrier, 3)

    @pl.loop(0, STRIPS // 2)
    def _(i):
        from_x(s, 2 * i + r).start()

    @pl.loop(0, STRIPS)
    def _(b):
        k, _ = strip(b)
        from_core(s, k).start()
        mine(k).start()

    @pl.loop(0, NT)
    def _(t):
        copies(x_h, a_v, load, t).wait()
        tile(a_v, t)[...] = normed(tile(a_v, t)[...])
        copies(a_v, a_h, a_out, t).start()

    def arrive(b):
        k, along_x = strip(b)

        @pl.when(along_x == 1)
        def _():
            from_x(by_x, k).wait_recv()
            from_y(by_x, k).start()
            handed_on(by_x, k).start()

        @pl.when(along_x == 0)
        def _():
            from_y(by_x, k).wait_recv()
            handed_on(by_x, k).start()

    arrive(0)

    @pl.loop(0, STRIPS)
    def _(b):
        k, _ = strip(b)
        mine(k).wait()
        from_core(by_core, k).wait_recv()
        handed_on(far, k).wait_recv()
        kept(k).start()

        def head(t, slot):
            a = tile(a_v, t)[...]
            gate_s[slot][...] = dot(a, full[:, k, 0].reshape(D, W))
            up_s[slot][...] = dot(a, full[:, k, 1].reshape(D, W))

        def tail(t, slot):
            for q in range(0, T, ROWS):
                gate = gate_s[slot][q : q + ROWS]
                act_s[q : q + ROWS] = (gate * jax.nn.sigmoid(gate) * up_s[slot][q : q + ROWS]).astype(BF16)
            old = jnp.where(b == 0, 0.0, tile(y_v, t)[...])
            tile(y_v, t)[...] = old + dot(act_s[...], full[:, k, 2].reshape(W, D))

        def before(t, count):
            if not isinstance(t, int) or t != NT - 1:
                return

            @pl.when(b < STRIPS - 1)
            def _():
                arrive(b + 1)

        pipelined(head, tail, before, lambda t, count: None)

    for t in range(NT):
        copies(y_v, y_h, y_out, t).start()

    @pl.loop(0, STRIPS // 2)
    def _(i):
        from_x(s, 2 * i + r).wait_send()
        from_y(by_x, 2 * i + r).wait_send()

    @pl.loop(0, STRIPS)
    def _(k):
        from_core(s, k).wait_send()
        handed_on(by_x, k).wait_send()
        kept(k).wait()

    for t in range(NT):
        copies(a_v, a_h, a_out, t).wait()
        copies(y_v, y_h, y_out, t).wait()


def gather_fwd(x, pk):
    sem = lambda n: pltpu.SemaphoreType.DMA((n,))
    return pl.pallas_call(
        gather_kernel,
        out_shape=[jax.ShapeDtypeStruct((4, STRIPS, 3, 128, 512), BF16), ROW, jax.ShapeDtypeStruct((TOK, D), F32)],
        in_specs=[ANY] * 2,
        out_specs=[ANY] * 3,
        scratch_shapes=[pltpu.VMEM((4, STRIPS, 3, 128, 512), BF16), pltpu.VMEM((TOK, D), BF16), pltpu.VMEM((TOK, D), F32)]
        + [pltpu.VMEM((T, W), F32)] * 4 + [pltpu.VMEM((T, W), BF16)] + [sem(NT)] + [sem(STRIPS)] * 10 + [sem(NT)] * 2,
        compiler_params=pltpu.CompilerParams(vmem_limit_bytes=60 << 20, collective_id=0, has_side_effects=True),
        cost_estimate=pl.CostEstimate(flops=6 * TOK * D * W * STRIPS, bytes_accessed=80 << 20, transcendentals=TOK * W * STRIPS),
        name="gather_fwd",
    )(x, pk)


CHUNKS = 4


def adam_kernel(skip, *refs):
    adam_step(refs[skip : skip + 15], refs[skip + 15 : skip + 24])


def adam(l, j, gs, gr, weights, m, v, before):
    ins, outs = adam_specs(l, j)
    shapes = [jax.ShapeDtypeStruct(w.shape, dt) for dt in (BF16, F32, F32) for w in weights]
    before = list(before or [])
    return pl.pallas_call(
        functools.partial(adam_kernel, len(before)),
        grid=(4,),
        out_shape=shapes,
        in_specs=[ANY] * len(before) + ins,
        out_specs=outs,
        input_output_aliases={i: i for i in range(len(before))},
        cost_estimate=pl.CostEstimate(flops=10 * 3 * 4 * 128 * 512, bytes_accessed=18 << 20, transcendentals=3 * 4 * 128 * 512),
        name="adam",
    )(*before, *[gs] * 3, *[gr] * 3, *weights, *m, *v)


def solution(mesh):
    pairs = [(0, 1), (1, 0)]

    def step(x, dy, *arrays):
        weights, m, v = (arrays[i : i + 3] for i in (0, 3, 6))
        x, dy = x[0], dy[0]
        early, *rest = pack(1, ((0, 1), (1, 2), (2, 4)), *weights)
        parts = [lax.all_gather(early, "s", axis=0)]
        full0, a0, y = gather_fwd(x, pack(0, ((0, 4),), *weights)[0])
        parts += [lax.all_gather(one, "s", axis=0) for one in rest]
        full1 = [(parts[0], 0), (parts[1], 0), (parts[2], 0), (parts[2], 4)]
        h1, a1, a1T, dyT = rowwise(middle_kernel, [x, y, dy], [ROW, ROW, COL, COL])
        order = [(1, j) for j in range(CHUNKS)] + [(0, j) for j in range(CHUNKS)]
        ours, theirs, out, da = [], [], None, None
        for i, (l, j) in enumerate(order):
            deps, state = [], None
            if i >= 3:
                deps = [ours[i - 2]]
            if i >= 4:
                state = (*order[i - 4], ours[i - 4], theirs[i - 4], weights, m, v, out)
            if (l, j) == (0, 0):
                dh, dhT, a0T = rowwise(back_kernel, [h1, dy, da, a0], [ROW, COL, COL])
            if i >= 2:
                theirs.append(lax.ppermute(ours[i - 2], "r", pairs))
            if l == 1:
                term, da, *new = bwd(a1, dy, a1T, dyT, *full1[j], da, deps=deps, state=state)
            else:
                term, *new = bwd(a0, dh, a0T, dhT, full0, 4 * j, need=False, deps=deps, state=state)
            if state:
                out = new
            ours.append(lax.psum_scatter(term, "s", scatter_dimension=0, tiled=True)[0])
        last = len(order) - 1
        theirs.append(lax.ppermute(ours[last - 1], "r", pairs))
        for i in range(last - 3, last):
            out = adam(*order[i], ours[i], theirs[i], weights, m, v, out)
        theirs.append(lax.ppermute(ours[last], "r", pairs))
        out = adam(*order[last], ours[last], theirs[last], weights, m, v, out)
        return tuple(out)

    states, cut = P(("rep", "r", "s"), None, None), P(None, "s", None)
    return jax.shard_map(
        step,
        mesh=mesh,
        in_specs=(states, states) + (cut,) * 9,
        out_specs=(P("rep", "s", None),) * 9,
        check_vma=False,
    )
```

```python
import functools
import jax, jax.numpy as jnp
from jax import lax
from jax.experimental import pallas as pl
from jax.experimental.pallas import tpu as pltpu
from jax.sharding import PartitionSpec as P

F32, BF16 = jnp.float32, jnp.bfloat16
TOK, D, W = 4096, 512, 512
T = 512
NT = TOK // T
ROWS = 32
ANY = pl.BlockSpec(memory_space=pl.ANY)
STRIP = pl.BlockSpec((4, 1, 3, 128, 512), lambda k: (0, k, 0, 0, 0))


def dot(a, b):
    return jnp.dot(a, b, preferred_element_type=F32)


def dot_t(a, b):
    return lax.dot_general(a, b, (((0,), (0,)), ((), ())), preferred_element_type=F32)


def tile(ref, t):
    return ref.at[pl.ds(pl.multiple_of(t * T, T), T), :]


def copies(src, dst, sem, t):
    return pltpu.make_async_copy(tile(src, t), tile(dst, t), sem.at[t])


def pipelined(head, tail, before, after):
    before(0, 1)
    head(0, 0)

    @pl.loop(0, NT // 2 - 1)
    def _(i):
        before(2 * i + 1, 2)
        head(2 * i + 1, 1)
        tail(2 * i, 0)
        head(2 * i + 2, 0)
        tail(2 * i + 1, 1)
        after(2 * i, 2)

    before(NT - 1, 1)
    head(NT - 1, 1)
    tail(NT - 2, 0)
    tail(NT - 1, 1)


def adamw(w, m, v, g):
    m = 0.9 * m + 0.1 * g
    v = 0.95 * v + 0.05 * g * g
    step = m * lax.rsqrt(v + 1e-8) + 0.1 * w
    return (w - 0.02 * step).astype(BF16), m, v


def adam_step(ins, outs):
    gs, gr, w, m, v = (ins[3 * i : 3 * i + 3] for i in range(5))
    for which in range(3):
        g = (gs[which][...].astype(F32) + gr[which][...].astype(F32)).astype(BF16).astype(F32)
        for k in range(g.shape[0]):
            c = slice(128 * k, 128 * (k + 1)) if which < 2 else slice(0, D)
            new = adamw(w[which][0, :, c].astype(F32), m[which][0, :, c], v[which][0, :, c], g[k, 0])
            for i in range(3):
                outs[3 * i + which][0, :, c] = new[i]


def adam_specs(l, q, n, at):
    cols = [pl.BlockSpec((n, 1, 128, 128), functools.partial(lambda which, i: (at // n, which, 0, i), which)) for which in range(2)]
    cols.append(pl.BlockSpec((1, 1, 32 * n, D), lambda i: (at + i * n // 4, 2, i % (4 // n), 0)))
    own = [pl.BlockSpec((1, 128, 128 * n), lambda i: (l, 0, i * (16 // n) + q // n))] * 2
    own.append(pl.BlockSpec((1, 32 * n, D), lambda i: (l, q * 4 // n + i, 0)))
    return cols * 2 + own * 3, own * 3


def bwd_kernel(n, need, first, state, skip, *refs):
    refs = list(refs)
    take = lambda count: [refs.pop(0) for _ in range(count)]
    take(skip)
    ad_in = take(15) if state else []
    a_h, dy_h = take(2)
    da_h = take(1)[0] if need and not first else None
    p = refs.pop(0)
    g = refs.pop(0)
    out_h = refs.pop(0) if need else None
    ad_out = take(9) if state else []
    a_v, dy_v, act_v, dgu_v, wT, wdT = take(6)
    gate_s, up_s, dact_s = take(2), take(2), take(2)
    da_v = refs.pop(0) if need else None
    sa, sd = take(2)
    sp, so = take(2) if need else (None, None)
    k = pl.program_id(0)

    @pl.when(k == 0)
    def _():
        for t in range(NT):
            copies(a_h, a_v, sa, t).start()
            copies(dy_h, dy_v, sd, t).start()
            if need and not first:
                copies(da_h, da_v, sp, t).start()

    def before(t, count):
        @pl.when(k == 0)
        def _():
            for i in range(count):
                copies(a_h, a_v, sa, t + i).wait()
                copies(dy_h, dy_v, sd, t + i).wait()
                if need and not first:
                    copies(da_h, da_v, sp, t + i).wait()

    def head(t, slot):
        a = tile(a_v, t)[...]
        gate_s[slot][...] = dot(a, p[:, 0, 0].reshape(D, W))
        up_s[slot][...] = dot(a, p[:, 0, 1].reshape(D, W))
        dact_s[slot][...] = dot(tile(dy_v, t)[...], wdT[...]).astype(BF16)

    def tail(t, slot):
        for r in range(0, T, ROWS):
            rows = slice(r, r + ROWS)
            here = pl.ds(pl.multiple_of(t * T + r, ROWS), ROWS)
            gate, up, dact = gate_s[slot][rows], up_s[slot][rows], dact_s[slot][rows].astype(F32)
            sig = jax.nn.sigmoid(gate)
            silu = gate * sig
            act_v[here] = (silu * up).astype(BF16)
            dgu_v[here, W:] = (dact * silu).astype(BF16)
            dgu_v[here, :W] = (dact * up * (sig + silu * (1 - sig))).astype(BF16)
        if need:
            old = tile(da_v, t)[...]
            if first:
                old = jnp.where(k == 0, 0.0, old)
            tile(da_v, t)[...] = old + dot(tile(dgu_v, t)[...], wT[...])

    def after(t, count):
        if need:
            @pl.when(k == n - 1)
            def _():
                for i in range(count):
                    copies(da_v, out_h, so, t + i).start()

    wdT[...] = p[:, 0, 2].reshape(W, D).T
    if need:
        wT[:W] = p[:, 0, 0].reshape(D, W).T
        wT[W:] = p[:, 0, 1].reshape(D, W).T
    pipelined(head, tail, before, after)
    after(NT - 2, 2)

    for which in range(2):
        g[:, 0, which] = dot_t(a_v[...], dgu_v[:, W * which : W * (which + 1)]).astype(BF16).reshape(4, 128, W)
    g[:, 0, 2] = dot_t(act_v[...], dy_v[...]).astype(BF16).reshape(4, 128, D)
    if state:
        adam_step(ad_in, ad_out)

    if need:
        @pl.when(k == n - 1)
        def _():
            for t in range(NT):
                copies(da_v, out_h, so, t).wait()


def bwd(a, dy, p, at, n, da=None, need=True, state=None):
    first = da is None
    sem = pltpu.SemaphoreType.DMA((NT,))
    args, specs = [], []
    out_shapes = [jax.ShapeDtypeStruct((4, n, 3, 128, 512), BF16)]
    out_specs = [STRIP]
    if need:
        out_shapes.append(jax.ShapeDtypeStruct((TOK, D), F32))
        out_specs.append(ANY)
    aliases = {}
    if state:
        where, gs, gr, weights, m, v, before = state
        before = list(before or [])
        aliases = {len(args) + i: len(out_shapes) + i for i in range(len(before))}
        args += before
        specs += [ANY] * len(before)
    skip = len(args)
    if state:
        ins, outs = adam_specs(*where)
        args += [gs] * 3 + [gr] * 3 + [*weights, *m, *v]
        specs += ins
        out_shapes += [jax.ShapeDtypeStruct(w.shape, dt) for dt in (BF16, F32, F32) for w in weights]
        out_specs += outs
    rest = [a, dy] + ([da] if need and not first else [])
    args += rest + [p]
    specs += [ANY] * len(rest) + [pl.BlockSpec((4, 1, 3, 128, 512), lambda k: (0, at + k, 0, 0, 0))]
    big = lambda dt: pltpu.VMEM((TOK, D), dt)
    return pl.pallas_call(
        functools.partial(bwd_kernel, n, need, first, bool(state), skip),
        grid=(n,),
        out_shape=out_shapes,
        in_specs=specs,
        out_specs=out_specs,
        scratch_shapes=[big(BF16)] * 2 + [big(BF16), pltpu.VMEM((TOK, 2 * W), BF16), pltpu.VMEM((2 * W, D), BF16), pltpu.VMEM((D, W), BF16)]
        + [pltpu.VMEM((T, W), F32)] * 4 + [pltpu.VMEM((T, W), BF16)] * 2
        + ([big(F32)] if need else []) + [sem] * 2 + ([sem] * 2 if need else []),
        input_output_aliases=aliases,
        compiler_params=pltpu.CompilerParams(vmem_limit_bytes=63 << 20, dimension_semantics=("arbitrary",)),
        cost_estimate=pl.CostEstimate(flops=2 * (8 if need else 6) * TOK * D * W * n, bytes_accessed=n * 6 * (1 << 19) + (20 << 20), transcendentals=TOK * W * n),
        name="bwd",
    )(*args)


def normed(h):
    wide = h.astype(F32)
    scale = lax.rsqrt(jnp.mean(wide**2, -1, keepdims=True) + 1e-6)
    return (wide * scale).astype(BF16)


def rowwise(body, ins, outs):
    spec = pl.BlockSpec((T, D), lambda t: (t, 0))
    return pl.pallas_call(
        body,
        grid=(NT,),
        out_shape=outs,
        in_specs=[spec] * len(ins),
        out_specs=[spec] * len(outs),
        cost_estimate=pl.CostEstimate(flops=20 * TOK * D, bytes_accessed=24 << 20, transcendentals=TOK),
    )(*ins)


ROW = jax.ShapeDtypeStruct((TOK, D), BF16)


def middle_kernel(x, y, h, a):
    h[...] = (x[...].astype(F32) + y[...].astype(BF16).astype(F32)).astype(BF16)
    a[...] = normed(h[...])


def back_kernel(h, dy, da, dh):
    wide = h[...].astype(F32)
    scale = lax.rsqrt(jnp.mean(wide**2, -1, keepdims=True) + 1e-6)
    by_a = da[...].astype(BF16).astype(F32)
    by_h = by_a * scale - wide * (scale * scale * scale * jnp.mean(by_a * wide, -1, keepdims=True))
    dh[...] = (dy[...].astype(F32) + by_h.astype(BF16).astype(F32)).astype(BF16)


STRIPS = 16


def pack_kernel(base, *refs):
    gates, ups, down = refs[:4], refs[4:8], refs[8]
    outs = refs[9:]
    for i, (lo, hi) in enumerate(base):
        @pl.when((pl.program_id(0) >= lo) & (pl.program_id(0) < hi))
        def _(out=outs[i]):
            for k in range(4):
                for which, parts in ((0, gates), (1, ups)):
                    for s in range(4):
                        out[k, which, :, 128 * s : 128 * (s + 1)] = parts[s][0, :, 128 * k : 128 * (k + 1)]
                out[k, 2] = down[0, 128 * k : 128 * (k + 1), :]


def pack(l, base, w_gate, w_up, w_down):
    wide = [pl.BlockSpec((1, 128, 512), functools.partial(lambda s, j: (l, 0, 4 * s + j), s)) for s in range(4)]
    return pl.pallas_call(
        functools.partial(pack_kernel, base),
        grid=(4,),
        out_shape=[jax.ShapeDtypeStruct((4 * (hi - lo), 3, 128, 512), BF16) for lo, hi in base],
        in_specs=wide + wide + [pl.BlockSpec((1, 512, 512), lambda j: (l, j, 0))],
        out_specs=[pl.BlockSpec((4, 3, 128, 512), functools.partial(lambda lo, hi, j: (jnp.clip(j - lo, 0, hi - lo - 1), 0, 0, 0), lo, hi)) for lo, hi in base],
        cost_estimate=pl.CostEstimate(flops=1 << 21, bytes_accessed=12 << 20, transcendentals=0),
        name="pack",
    )(*[w_gate] * 4, *[w_up] * 4, w_down)


def gather_kernel(x_h, pk, full_h, a_h, y_h, full, a_v, y_v, g0, u0, g1, u1, act_s, *sems):
    load, own, x_send, x_recv, y_send, y_recv, own_send, own_recv, on_send, on_recv, put, a_out, y_out = sems
    gate_s, up_s = (g0, g1), (u0, u1)
    s, r = lax.axis_index("s"), lax.axis_index("r")
    by_x, by_core = lax.rem(s + 2, 4), s + 1 - 2 * lax.rem(s, 2)
    far = lax.rem(by_core + 2, 4)

    def remote(src, block, k, send, recv, where):
        return pltpu.make_async_remote_copy(
            src_ref=src, dst_ref=full.at[block, k], send_sem=send.at[k], recv_sem=recv.at[k],
            device_id=where, device_id_type=pl.DeviceIdType.MESH,
        )

    def strip(b):
        odd, first, last = lax.rem(b, 2), (15 - b) // 15, b // 15
        return odd * (b + 1 + r) + (1 - odd) * (b - 1 - r) + (first - last) * (1 + 2 * r), odd * (1 - last) + first

    def from_x(block, k):
        return remote(pk.at[k], block, k, x_send, x_recv, {"s": by_x})

    def from_y(block, k):
        return remote(full.at[block, k], block, k, y_send, y_recv, {"r": 1 - r})

    def from_core(block, k):
        return remote(pk.at[k], block, k, own_send, own_recv, {"s": by_core})

    def handed_on(block, k):
        return remote(full.at[block, k], block, k, on_send, on_recv, {"s": by_core})

    def mine(k):
        return pltpu.make_async_copy(pk.at[k], full.at[s, k], own.at[k])

    def kept(k):
        return pltpu.make_async_copy(full.at[:, k], full_h.at[:, k], put.at[k])

    for t in range(NT):
        copies(x_h, a_v, load, t).start()
    barrier = pltpu.get_barrier_semaphore()
    for where in ({"s": by_x}, {"s": by_core}, {"r": 1 - r}):
        pl.semaphore_signal(barrier, inc=1, device_id=where, device_id_type=pl.DeviceIdType.MESH)
    pl.semaphore_wait(barrier, 3)

    @pl.loop(0, STRIPS // 2)
    def _(i):
        from_x(s, 2 * i + r).start()

    @pl.loop(0, STRIPS)
    def _(b):
        k, _ = strip(b)
        from_core(s, k).start()
        mine(k).start()

    @pl.loop(0, NT)
    def _(t):
        copies(x_h, a_v, load, t).wait()
        tile(a_v, t)[...] = normed(tile(a_v, t)[...])
        copies(a_v, a_h, a_out, t).start()

    def arrive(b):
        k, along_x = strip(b)

        @pl.when(along_x == 1)
        def _():
            from_x(by_x, k).wait_recv()
            from_y(by_x, k).start()
            handed_on(by_x, k).start()

        @pl.when(along_x == 0)
        def _():
            from_y(by_x, k).wait_recv()
            handed_on(by_x, k).start()

    arrive(0)

    @pl.loop(0, STRIPS)
    def _(b):
        k, _ = strip(b)
        mine(k).wait()
        from_core(by_core, k).wait_recv()
        handed_on(far, k).wait_recv()
        kept(k).start()

        def head(t, slot):
            a = tile(a_v, t)[...]
            gate_s[slot][...] = dot(a, full[:, k, 0].reshape(D, W))
            up_s[slot][...] = dot(a, full[:, k, 1].reshape(D, W))

        def tail(t, slot):
            for q in range(0, T, ROWS):
                gate = gate_s[slot][q : q + ROWS]
                act_s[q : q + ROWS] = (gate * jax.nn.sigmoid(gate) * up_s[slot][q : q + ROWS]).astype(BF16)
            old = jnp.where(b == 0, 0.0, tile(y_v, t)[...])
            tile(y_v, t)[...] = old + dot(act_s[...], full[:, k, 2].reshape(W, D))

        def before(t, count):
            if not isinstance(t, int) or t != NT - 1:
                return

            @pl.when(b < STRIPS - 1)
            def _():
                arrive(b + 1)

        pipelined(head, tail, before, lambda t, count: None)

    for t in range(NT):
        copies(y_v, y_h, y_out, t).start()

    @pl.loop(0, STRIPS // 2)
    def _(i):
        from_x(s, 2 * i + r).wait_send()
        from_y(by_x, 2 * i + r).wait_send()

    @pl.loop(0, STRIPS)
    def _(k):
        from_core(s, k).wait_send()
        handed_on(by_x, k).wait_send()
        kept(k).wait()

    for t in range(NT):
        copies(a_v, a_h, a_out, t).wait()
        copies(y_v, y_h, y_out, t).wait()


def gather_fwd(x, pk):
    sem = lambda n: pltpu.SemaphoreType.DMA((n,))
    return pl.pallas_call(
        gather_kernel,
        out_shape=[jax.ShapeDtypeStruct((4, STRIPS, 3, 128, 512), BF16), ROW, jax.ShapeDtypeStruct((TOK, D), F32)],
        in_specs=[ANY] * 2,
        out_specs=[ANY] * 3,
        scratch_shapes=[pltpu.VMEM((4, STRIPS, 3, 128, 512), BF16), pltpu.VMEM((TOK, D), BF16), pltpu.VMEM((TOK, D), F32)]
        + [pltpu.VMEM((T, W), F32)] * 4 + [pltpu.VMEM((T, W), BF16)] + [sem(NT)] + [sem(STRIPS)] * 10 + [sem(NT)] * 2,
        compiler_params=pltpu.CompilerParams(vmem_limit_bytes=60 << 20, collective_id=0, has_side_effects=True),
        cost_estimate=pl.CostEstimate(flops=6 * TOK * D * W * STRIPS, bytes_accessed=80 << 20, transcendentals=TOK * W * STRIPS),
        name="gather_fwd",
    )(x, pk)


def adam_kernel(skip, *refs):
    adam_step(refs[skip : skip + 15], refs[skip + 15 :])


def adam(where, gs, gr, weights, m, v, before):
    ins, outs = adam_specs(*where)
    n = where[2]
    return pl.pallas_call(
        functools.partial(adam_kernel, len(before)),
        grid=(4,),
        out_shape=[jax.ShapeDtypeStruct(w.shape, dt) for dt in (BF16, F32, F32) for w in weights],
        in_specs=[ANY] * len(before) + ins,
        out_specs=outs,
        input_output_aliases={i: i for i in range(len(before))},
        cost_estimate=pl.CostEstimate(flops=10 * 3 * n * 128 * 512, bytes_accessed=(18 << 20) * n // 4, transcendentals=3 * n * 128 * 512),
        name="adam",
    )(*before, *[gs] * 3, *[gr] * 3, *weights, *m, *v)


CALLS = ((1, 0, 4), (1, 4, 4), (1, 8, 4), (1, 12, 4), (0, 0, 4), (0, 4, 4), (0, 8, 4), (0, 12, 2), (0, 14, 2))
SWAPS = {i: i - 2 for i in range(2, 8)}
RIDES = {4: 0, 5: 1, 6: 2}


def solution(mesh):
    pairs = [(0, 1), (1, 0)]

    def step(x, dy, *arrays):
        weights, m, v = (arrays[i : i + 3] for i in (0, 3, 6))
        x, dy = x[0], dy[0]
        ours, theirs, out, da = [], {}, [], None

        def swap(i):
            theirs[i] = lax.ppermute(ours[i], "r", pairs)

        def state(i):
            return (*CALLS[i], 0), ours[i], theirs[i], weights, m, v, out

        early, *rest = pack(1, ((0, 1), (1, 2), (2, 4)), *weights)
        parts = [lax.all_gather(early, "s", axis=0)]
        full0, a0, y = gather_fwd(x, pack(0, ((0, 4),), *weights)[0])
        parts += [lax.all_gather(one, "s", axis=0) for one in rest]
        h1, a1 = rowwise(middle_kernel, [x, y], [ROW, ROW])
        for i, (l, q, n) in enumerate(CALLS):
            if (l, q) == (0, 0):
                dh = rowwise(back_kernel, [h1, dy, da], [ROW])[0]
            if i in SWAPS:
                swap(SWAPS[i])
            ride = state(RIDES[i]) if i in RIDES else None
            if l == 1:
                term, da, *new = bwd(a1, dy, parts[min(i, 2)], 4 if i == 3 else 0, n, da, state=ride)
            else:
                term, *new = bwd(a0, dh, full0, q, n, need=False, state=ride)
            if ride:
                out = new
            ours.append(lax.psum_scatter(term, "s", scatter_dimension=0, tiled=True)[0])
        swap(6)
        out = adam(*state(3))
        swap(7)
        out = adam(*state(4))
        out = adam(*state(5))
        swap(8)
        for i in (6, 7, 8):
            out = adam(*state(i))
        return tuple(out)

    states, cut = P(("rep", "r", "s"), None, None), P(None, "s", None)
    return jax.shard_map(
        step,
        mesh=mesh,
        in_specs=(states, states) + (cut,) * 9,
        out_specs=(P("rep", "s", None),) * 9,
        check_vma=False,
    )
```

```python
import functools
import jax, jax.numpy as jnp
from jax import lax
from jax.experimental import pallas as pl
from jax.experimental.pallas import tpu as pltpu
from jax.sharding import PartitionSpec as P

F32, BF16 = jnp.float32, jnp.bfloat16
TOK, D, W = 4096, 512, 512
T = 512
NT = TOK // T
ROWS = 32
ANY = pl.BlockSpec(memory_space=pl.ANY)
STRIP = pl.BlockSpec((4, 1, 3, 128, 512), lambda k: (0, k, 0, 0, 0))


def dot(a, b):
    return jnp.dot(a, b, preferred_element_type=F32)


def dot_t(a, b):
    return lax.dot_general(a, b, (((0,), (0,)), ((), ())), preferred_element_type=F32)


def tile(ref, t):
    return ref.at[pl.ds(pl.multiple_of(t * T, T), T), :]


def copies(src, dst, sem, t):
    return pltpu.make_async_copy(tile(src, t), tile(dst, t), sem.at[t])


def pipelined(head, tail, before, after):
    before(0, 1)
    head(0, 0)

    @pl.loop(0, NT // 2 - 1)
    def _(i):
        before(2 * i + 1, 2)
        head(2 * i + 1, 1)
        tail(2 * i, 0)
        head(2 * i + 2, 0)
        tail(2 * i + 1, 1)
        after(2 * i, 2)

    before(NT - 1, 1)
    head(NT - 1, 1)
    tail(NT - 2, 0)
    tail(NT - 1, 1)


def adamw(w, m, v, g):
    m = 0.9 * m + 0.1 * g
    v = 0.95 * v + 0.05 * g * g
    step = m * lax.rsqrt(v + 1e-8) + 0.1 * w
    return (w - 0.02 * step).astype(BF16), m, v


def normed(h):
    wide = h.astype(F32)
    scale = lax.rsqrt(jnp.mean(wide**2, -1, keepdims=True) + 1e-6)
    return (wide * scale).astype(BF16)


def by_input(h, dy, da):
    wide = h.astype(F32)
    scale = lax.rsqrt(jnp.mean(wide**2, -1, keepdims=True) + 1e-6)
    by_a = da.astype(BF16).astype(F32)
    by_h = by_a * scale - wide * (scale * scale * scale * jnp.mean(by_a * wide, -1, keepdims=True))
    return (dy.astype(F32) + by_h.astype(BF16).astype(F32)).astype(BF16)


def adam_step(ins, outs):
    gs, gr, w, m, v = (ins[3 * i : 3 * i + 3] for i in range(5))
    for which in range(3):
        g = (gs[which][...].astype(F32) + gr[which][...].astype(F32)).astype(BF16).astype(F32)
        for k in range(g.shape[0]):
            c = slice(128 * k, 128 * (k + 1)) if which < 2 else slice(0, D)
            new = adamw(w[which][0, :, c].astype(F32), m[which][0, :, c], v[which][0, :, c], g[k, 0])
            for i in range(3):
                outs[3 * i + which][0, :, c] = new[i]


def adam_specs(l, q, n, at):
    cols = [pl.BlockSpec((n, 1, 128, 128), functools.partial(lambda which, i: (at // n, which, 0, i), which)) for which in range(2)]
    cols.append(pl.BlockSpec((1, 1, 32 * n, D), lambda i: (at + i * n // 4, 2, i % (4 // n), 0)))
    own = [pl.BlockSpec((1, 128, 128 * n), lambda i: (l, 0, i * (16 // n) + q // n))] * 2
    own.append(pl.BlockSpec((1, 32 * n, D), lambda i: (l, q * 4 // n + i, 0)))
    return cols * 2 + own * 3, own * 3


def bwd_kernel(n, need, first, end, state, skip, *refs):
    refs = list(refs)
    take = lambda count: [refs.pop(0) for _ in range(count)]
    take(skip)
    ad_in = take(15) if state else []
    a_h, dy_h = take(2)
    da_h = take(1)[0] if need and not first else None
    h_h = take(1)[0] if end else None
    p = refs.pop(0)
    g = refs.pop(0)
    out_h = refs.pop(0) if need else None
    ad_out = take(9) if state else []
    a_v, dy_v, act_v, dgu_v, wT, wdT = take(6)
    gate_s, up_s, dact_s = take(2), take(2), take(2)
    da_v = refs.pop(0) if need else None
    h_v = refs.pop(0) if end else None
    sa, sd = take(2)
    sp, so = take(2) if need else (None, None)
    sh = refs.pop(0) if end else None
    k = pl.program_id(0)

    @pl.when(k == 0)
    def _():
        for t in range(NT):
            copies(a_h, a_v, sa, t).start()
            copies(dy_h, dy_v, sd, t).start()
            if need and not first:
                copies(da_h, da_v, sp, t).start()
            if end:
                copies(h_h, h_v, sh, t).start()

    def before(t, count):
        @pl.when(k == 0)
        def _():
            for i in range(count):
                copies(a_h, a_v, sa, t + i).wait()
                copies(dy_h, dy_v, sd, t + i).wait()
                if need and not first:
                    copies(da_h, da_v, sp, t + i).wait()

    def head(t, slot):
        a = tile(a_v, t)[...]
        gate_s[slot][...] = dot(a, p[:, 0, 0].reshape(D, W))
        up_s[slot][...] = dot(a, p[:, 0, 1].reshape(D, W))
        dact_s[slot][...] = dot(tile(dy_v, t)[...], wdT[...]).astype(BF16)

    def tail(t, slot):
        for r in range(0, T, ROWS):
            rows = slice(r, r + ROWS)
            here = pl.ds(pl.multiple_of(t * T + r, ROWS), ROWS)
            gate, up, dact = gate_s[slot][rows], up_s[slot][rows], dact_s[slot][rows].astype(F32)
            sig = jax.nn.sigmoid(gate)
            silu = gate * sig
            act_v[here] = (silu * up).astype(BF16)
            dgu_v[here, W:] = (dact * silu).astype(BF16)
            dgu_v[here, :W] = (dact * up * (sig + silu * (1 - sig))).astype(BF16)
        if need:
            old = tile(da_v, t)[...]
            if first:
                old = jnp.where(k == 0, 0.0, old)
            tile(da_v, t)[...] = old + dot(tile(dgu_v, t)[...], wT[...])

    def after(t, count):
        if need and not end:
            @pl.when(k == n - 1)
            def _():
                for i in range(count):
                    copies(da_v, out_h, so, t + i).start()

    wdT[...] = p[:, 0, 2].reshape(W, D).T
    if need:
        wT[:W] = p[:, 0, 0].reshape(D, W).T
        wT[W:] = p[:, 0, 1].reshape(D, W).T
    pipelined(head, tail, before, after)
    after(NT - 2, 2)

    for which in range(2):
        g[:, 0, which] = dot_t(a_v[...], dgu_v[:, W * which : W * (which + 1)]).astype(BF16).reshape(4, 128, W)
    g[:, 0, 2] = dot_t(act_v[...], dy_v[...]).astype(BF16).reshape(4, 128, D)
    if state:
        adam_step(ad_in, ad_out)

    if end:
        @pl.when(k == n - 1)
        def _():
            @pl.loop(0, NT)
            def _(t):
                copies(h_h, h_v, sh, t).wait()
                tile(h_v, t)[...] = by_input(tile(h_v, t)[...], tile(dy_v, t)[...], tile(da_v, t)[...])
                copies(h_v, out_h, so, t).start()

            for t in range(NT):
                copies(h_v, out_h, so, t).wait()
    elif need:
        @pl.when(k == n - 1)
        def _():
            for t in range(NT):
                copies(da_v, out_h, so, t).wait()


def bwd(a, dy, p, at, n, da=None, need=True, state=None, h=None):
    first, end = da is None, h is not None
    sem = pltpu.SemaphoreType.DMA((NT,))
    args, specs = [], []
    out_shapes = [jax.ShapeDtypeStruct((4, n, 3, 128, 512), BF16)]
    out_specs = [STRIP]
    if need:
        out_shapes.append(jax.ShapeDtypeStruct((TOK, D), BF16 if end else F32))
        out_specs.append(ANY)
    aliases = {}
    if state:
        where, gs, gr, weights, m, v, before = state
        before = list(before or [])
        aliases = {len(args) + i: len(out_shapes) + i for i in range(len(before))}
        args += before
        specs += [ANY] * len(before)
    skip = len(args)
    if state:
        ins, outs = adam_specs(*where)
        args += [gs] * 3 + [gr] * 3 + [*weights, *m, *v]
        specs += ins
        out_shapes += [jax.ShapeDtypeStruct(w.shape, dt) for dt in (BF16, F32, F32) for w in weights]
        out_specs += outs
    rest = [a, dy] + ([da] if need and not first else []) + ([h] if end else [])
    args += rest + [p]
    specs += [ANY] * len(rest) + [pl.BlockSpec((4, 1, 3, 128, 512), lambda k: (0, at + k, 0, 0, 0))]
    big = lambda dt: pltpu.VMEM((TOK, D), dt)
    return pl.pallas_call(
        functools.partial(bwd_kernel, n, need, first, end, bool(state), skip),
        grid=(n,),
        out_shape=out_shapes,
        in_specs=specs,
        out_specs=out_specs,
        scratch_shapes=[big(BF16)] * 2 + [big(BF16), pltpu.VMEM((TOK, 2 * W), BF16), pltpu.VMEM((2 * W, D), BF16), pltpu.VMEM((D, W), BF16)]
        + [pltpu.VMEM((T, W), F32)] * 4 + [pltpu.VMEM((T, W), BF16)] * 2
        + ([big(F32)] if need else []) + ([big(BF16)] if end else []) + [sem] * (2 + 2 * need + end),
        input_output_aliases=aliases,
        compiler_params=pltpu.CompilerParams(vmem_limit_bytes=63 << 20, dimension_semantics=("arbitrary",)),
        cost_estimate=pl.CostEstimate(flops=2 * (8 if need else 6) * TOK * D * W * n, bytes_accessed=n * 6 * (1 << 19) + (20 << 20), transcendentals=TOK * W * n),
        name="bwd",
    )(*args)


ROW = jax.ShapeDtypeStruct((TOK, D), BF16)


STRIPS = 16


def pack_kernel(base, *refs):
    gates, ups, down = refs[:4], refs[4:8], refs[8]
    outs = refs[9:]
    for i, (lo, hi) in enumerate(base):
        @pl.when((pl.program_id(0) >= lo) & (pl.program_id(0) < hi))
        def _(out=outs[i]):
            for k in range(4):
                for which, parts in ((0, gates), (1, ups)):
                    for s in range(4):
                        out[k, which, :, 128 * s : 128 * (s + 1)] = parts[s][0, :, 128 * k : 128 * (k + 1)]
                out[k, 2] = down[0, 128 * k : 128 * (k + 1), :]


def pack(l, base, w_gate, w_up, w_down):
    wide = [pl.BlockSpec((1, 128, 512), functools.partial(lambda s, j: (l, 0, 4 * s + j), s)) for s in range(4)]
    return pl.pallas_call(
        functools.partial(pack_kernel, base),
        grid=(4,),
        out_shape=[jax.ShapeDtypeStruct((4 * (hi - lo), 3, 128, 512), BF16) for lo, hi in base],
        in_specs=wide + wide + [pl.BlockSpec((1, 512, 512), lambda j: (l, j, 0))],
        out_specs=[pl.BlockSpec((4, 3, 128, 512), functools.partial(lambda lo, hi, j: (jnp.clip(j - lo, 0, hi - lo - 1), 0, 0, 0), lo, hi)) for lo, hi in base],
        cost_estimate=pl.CostEstimate(flops=1 << 21, bytes_accessed=12 << 20, transcendentals=0),
        name="pack",
    )(*[w_gate] * 4, *[w_up] * 4, w_down)


def gather_kernel(x_h, pk, full_h, a_h, h_h, next_h, full, x_v, a_v, y_v, g0, u0, g1, u1, act_s, *sems):
    load, own, x_send, x_recv, y_send, y_recv, own_send, own_recv, on_send, on_recv, put, a_out, h_out, next_out = sems
    gate_s, up_s = (g0, g1), (u0, u1)
    s, r = lax.axis_index("s"), lax.axis_index("r")
    by_x, by_core = lax.rem(s + 2, 4), s + 1 - 2 * lax.rem(s, 2)
    far = lax.rem(by_core + 2, 4)

    def remote(src, block, k, send, recv, where):
        return pltpu.make_async_remote_copy(
            src_ref=src, dst_ref=full.at[block, k], send_sem=send.at[k], recv_sem=recv.at[k],
            device_id=where, device_id_type=pl.DeviceIdType.MESH,
        )

    def strip(b):
        odd, first, last = lax.rem(b, 2), (15 - b) // 15, b // 15
        return odd * (b + 1 + r) + (1 - odd) * (b - 1 - r) + (first - last) * (1 + 2 * r), odd * (1 - last) + first

    def from_x(block, k):
        return remote(pk.at[k], block, k, x_send, x_recv, {"s": by_x})

    def from_y(block, k):
        return remote(full.at[block, k], block, k, y_send, y_recv, {"r": 1 - r})

    def from_core(block, k):
        return remote(pk.at[k], block, k, own_send, own_recv, {"s": by_core})

    def handed_on(block, k):
        return remote(full.at[block, k], block, k, on_send, on_recv, {"s": by_core})

    def mine(k):
        return pltpu.make_async_copy(pk.at[k], full.at[s, k], own.at[k])

    def kept(k):
        return pltpu.make_async_copy(full.at[:, k], full_h.at[:, k], put.at[k])

    for t in range(NT):
        copies(x_h, x_v, load, t).start()
    barrier = pltpu.get_barrier_semaphore()
    for where in ({"s": by_x}, {"s": by_core}, {"r": 1 - r}):
        pl.semaphore_signal(barrier, inc=1, device_id=where, device_id_type=pl.DeviceIdType.MESH)
    pl.semaphore_wait(barrier, 3)

    @pl.loop(0, STRIPS // 2)
    def _(i):
        from_x(s, 2 * i + r).start()

    @pl.loop(0, STRIPS)
    def _(b):
        k, _ = strip(b)
        from_core(s, k).start()
        mine(k).start()

    @pl.loop(0, NT)
    def _(t):
        copies(x_h, x_v, load, t).wait()
        tile(a_v, t)[...] = normed(tile(x_v, t)[...])
        copies(a_v, a_h, a_out, t).start()

    def arrive(b):
        k, along_x = strip(b)

        @pl.when(along_x == 1)
        def _():
            from_x(by_x, k).wait_recv()
            from_y(by_x, k).start()
            handed_on(by_x, k).start()

        @pl.when(along_x == 0)
        def _():
            from_y(by_x, k).wait_recv()
            handed_on(by_x, k).start()

    arrive(0)

    @pl.loop(0, STRIPS)
    def _(b):
        k, _ = strip(b)
        mine(k).wait()
        from_core(by_core, k).wait_recv()
        handed_on(far, k).wait_recv()
        kept(k).start()

        def head(t, slot):
            a = tile(a_v, t)[...]
            gate_s[slot][...] = dot(a, full[:, k, 0].reshape(D, W))
            up_s[slot][...] = dot(a, full[:, k, 1].reshape(D, W))

        def tail(t, slot):
            for q in range(0, T, ROWS):
                gate = gate_s[slot][q : q + ROWS]
                act_s[q : q + ROWS] = (gate * jax.nn.sigmoid(gate) * up_s[slot][q : q + ROWS]).astype(BF16)
            old = jnp.where(b == 0, 0.0, tile(y_v, t)[...])
            tile(y_v, t)[...] = old + dot(act_s[...], full[:, k, 2].reshape(W, D))

        def before(t, count):
            if not isinstance(t, int) or t != NT - 1:
                return

            @pl.when(b < STRIPS - 1)
            def _():
                arrive(b + 1)

        pipelined(head, tail, before, lambda t, count: None)

    @pl.loop(0, NT)
    def _(t):
        copies(a_v, a_h, a_out, t).wait()
        h = (tile(x_v, t)[...].astype(F32) + tile(y_v, t)[...].astype(BF16).astype(F32)).astype(BF16)
        tile(x_v, t)[...] = h
        tile(a_v, t)[...] = normed(h)
        copies(x_v, h_h, h_out, t).start()
        copies(a_v, next_h, next_out, t).start()

    @pl.loop(0, STRIPS // 2)
    def _(i):
        from_x(s, 2 * i + r).wait_send()
        from_y(by_x, 2 * i + r).wait_send()

    @pl.loop(0, STRIPS)
    def _(k):
        from_core(s, k).wait_send()
        handed_on(by_x, k).wait_send()
        kept(k).wait()

    for t in range(NT):
        copies(x_v, h_h, h_out, t).wait()
        copies(a_v, next_h, next_out, t).wait()


def gather_fwd(x, pk):
    sem = lambda n: pltpu.SemaphoreType.DMA((n,))
    return pl.pallas_call(
        gather_kernel,
        out_shape=[jax.ShapeDtypeStruct((4, STRIPS, 3, 128, 512), BF16), ROW, ROW, ROW],
        in_specs=[ANY] * 2,
        out_specs=[ANY] * 4,
        scratch_shapes=[pltpu.VMEM((4, STRIPS, 3, 128, 512), BF16), pltpu.VMEM((TOK, D), BF16), pltpu.VMEM((TOK, D), BF16), pltpu.VMEM((TOK, D), F32)]
        + [pltpu.VMEM((T, W), F32)] * 4 + [pltpu.VMEM((T, W), BF16)] + [sem(NT)] + [sem(STRIPS)] * 10 + [sem(NT)] * 3,
        compiler_params=pltpu.CompilerParams(vmem_limit_bytes=60 << 20, collective_id=0, has_side_effects=True),
        cost_estimate=pl.CostEstimate(flops=6 * TOK * D * W * STRIPS, bytes_accessed=80 << 20, transcendentals=TOK * W * STRIPS),
        name="gather_fwd",
    )(x, pk)


def adam_kernel(skip, *refs):
    adam_step(refs[skip : skip + 15], refs[skip + 15 :])


def adam(where, gs, gr, weights, m, v, before):
    ins, outs = adam_specs(*where)
    n = where[2]
    return pl.pallas_call(
        functools.partial(adam_kernel, len(before)),
        grid=(4,),
        out_shape=[jax.ShapeDtypeStruct(w.shape, dt) for dt in (BF16, F32, F32) for w in weights],
        in_specs=[ANY] * len(before) + ins,
        out_specs=outs,
        input_output_aliases={i: i for i in range(len(before))},
        cost_estimate=pl.CostEstimate(flops=10 * 3 * n * 128 * 512, bytes_accessed=(18 << 20) * n // 4, transcendentals=3 * n * 128 * 512),
        name="adam",
    )(*before, *[gs] * 3, *[gr] * 3, *weights, *m, *v)


CALLS = ((1, 0, 4), (1, 4, 4), (1, 8, 4), (1, 12, 4), (0, 0, 4), (0, 4, 4), (0, 8, 4), (0, 12, 2), (0, 14, 2))
SWAPS = {i: i - 2 for i in range(2, 8)}
RIDES = {4: 0, 5: 1, 6: 2}


def solution(mesh):
    pairs = [(0, 1), (1, 0)]

    def step(x, dy, *arrays):
        weights, m, v = (arrays[i : i + 3] for i in (0, 3, 6))
        x, dy = x[0], dy[0]
        ours, theirs, out, da = [], {}, [], None

        def swap(i):
            theirs[i] = lax.ppermute(ours[i], "r", pairs)

        def state(i):
            return (*CALLS[i], 0), ours[i], theirs[i], weights, m, v, out

        early, *rest = pack(1, ((0, 1), (1, 2), (2, 4)), *weights)
        parts = [lax.all_gather(early, "s", axis=0)]
        full0, a0, h1, a1 = gather_fwd(x, pack(0, ((0, 4),), *weights)[0])
        parts += [lax.all_gather(one, "s", axis=0) for one in rest]
        for i, (l, q, n) in enumerate(CALLS):
            if i in SWAPS:
                swap(SWAPS[i])
            ride = state(RIDES[i]) if i in RIDES else None
            if l == 1:
                term, da, *new = bwd(a1, dy, parts[min(i, 2)], 4 if i == 3 else 0, n, da, state=ride, h=h1 if q == 12 else None)
            else:
                term, *new = bwd(a0, da, full0, q, n, need=False, state=ride)
            if ride:
                out = new
            ours.append(lax.psum_scatter(term, "s", scatter_dimension=0, tiled=True)[0])
        swap(6)
        out = adam(*state(3))
        swap(7)
        out = adam(*state(4))
        out = adam(*state(5))
        swap(8)
        for i in (6, 7, 8):
            out = adam(*state(i))
        return tuple(out)

    states, cut = P(("rep", "r", "s"), None, None), P(None, "s", None)
    return jax.shard_map(
        step,
        mesh=mesh,
        in_specs=(states, states) + (cut,) * 9,
        out_specs=(P("rep", "s", None),) * 9,
        check_vma=False,
    )
```
